256 devices in a mesh: row: 32 (over y, x, core), col: 8 (over z).
Axes of the slice: x: 4, y: 4, z: 8, core: 2. Of those that a mesh axis runs over, the one named last changes fastest.
Arguments:
- vectors_window: float32 [32, 32, 64, 1024], P(None, 'row', None, 'col'), may hold values from -6 to 6
- column_strip: float32 [32, 32, 64, 1024], P(None, 'row', None, 'col'), may hold values from -6 to 6
- row_strip: float32 [1024, 64, 8, 128], P('row', None, 'col'), may hold values from -6 to 6
- factor: float32 [1024, 1024], P('row', 'col'), may hold values from -2 to 2
- window_start: int32 [1], replicated, may hold values from 1 to 64512
- deflated: int32 [1], replicated, may hold values from 0 to 512
Outputs:
- vectors_updated: float32 [32, 32, 64, 1024], P(None, 'row', None, 'col')
- column_updated: float32 [32, 32, 64, 1024], P(None, 'row', None, 'col')
- row_updated: float32 [1024, 64, 8, 128], P('row', None, 'col')
The draws below stay inside these ranges and needn't reach their ends.
All inputs are finite; a program needn't handle non-finite values.
Results may differ from the reference program's by a relative error of at most 0.0003.
Values sent between devices are 32-bit elements; how exact they have to be, the bound alone decides.
A program may use at most 64 MiB of HBM per device.

```python
import math
import jax
import jax.numpy as jnp
from jax import lax

W = 1024
BLK = 64
CBLK = 128
ROUNDS = 32
N = 65536
CROUNDS = 64
N_ROW = 32
N_COL = 8


def draw_factor(key, part):
    noise_key, scale_key = jax.random.split(key)
    positions = jnp.arange(W, dtype=jnp.float32) / (W - 1)
    spread = jnp.exp(jax.random.uniform(scale_key, (W,), jnp.float32, -1.15, 1.15))
    entries = jnp.clip(jax.random.normal(noise_key, (W, W), jnp.float32), -5.0, 5.0)
    column_scale = spread * jnp.exp(0.5 * math.log(3.0) * positions) / 1.5
    return (entries * column_scale[None, :] / math.sqrt(W)).astype(jnp.float32)


def block_levels(rng, dims, cuts, smallest, top_value):
    def one(dim, parts):
        steps = jax.random.uniform(jax.random.fold_in(jax.random.fold_in(rng, 6), dim), (parts,), jnp.float32, smallest / len(cuts), top_value / len(cuts))
        return jnp.repeat(jnp.exp(steps), dims[dim] // parts).reshape((-1,) + (1,) * (len(dims) - dim - 1))

    gain = one(*cuts[0])
    for cut in cuts[1:]:
        gain = gain * one(*cut)
    return gain


def normal_values(rng, shape, scale, most, shards=(), kind=jnp.bfloat16):
    gain = block_levels(rng, shape, shards, -0.22, 0.18) if shards else 1.0
    result = jax.random.normal(rng, shape, jnp.float32) * scale * gain
    return jnp.minimum(jnp.maximum(result, -most), most).astype(kind)


def setup_inputs(seed: int = 0) -> dict:
    streams_of = jax.random.split(jax.random.key(seed), 7)
    vectors_window = normal_values(streams_of[0], (ROUNDS, N_ROW, BLK, W), 1.0, 6.0, ((1, 32), (3, 8)), jnp.float32)
    column_strip = normal_values(streams_of[1], (ROUNDS, N_ROW, BLK, W), 1.0, 6.0, ((1, 32), (3, 8)), jnp.float32)
    row_strip = normal_values(streams_of[2], (W, CROUNDS, N_COL, CBLK), 1.0, 6.0, ((0, 32), (2, 8)), jnp.float32)
    factor = draw_factor(jax.random.fold_in(streams_of[6], 71), 0)
    window_start = jax.random.randint(streams_of[4], (1,), 1, N - W + 1).astype(jnp.int32)
    deflated = jax.random.randint(streams_of[5], (1,), 0, W // 2 + 1).astype(jnp.int32)
    return dict(vectors_window=vectors_window, column_strip=column_strip, row_strip=row_strip, factor=factor, window_start=window_start, deflated=deflated)


def reflect(factor, deflated):
    columns = jnp.arange(W, dtype=jnp.int32)
    kept_count = W - deflated[0]
    spike_row = jnp.where(columns < kept_count, factor[0], 0.0)
    squares = jnp.sum(spike_row * spike_row)
    corner = factor[0, 0]
    magnitude = jnp.sqrt(squares + 1e-06)
    signum = jnp.where(corner >= 0, 1.0, -1.0)
    vector = spike_row + jnp.where(columns == 0, signum * magnitude, 0.0)
    denominator = squares + 2.0 * jnp.abs(corner) * magnitude + magnitude * magnitude
    scaling = 2.0 / denominator
    reflected_image = jnp.dot(factor, vector, precision=lax.Precision.HIGHEST)
    return factor - scaling * reflected_image[:, None] * vector[None, :]

def reference(vectors_window, column_strip, row_strip, factor, window_start, deflated):
    highest = lax.Precision.HIGHEST
    rotation = reflect(factor, deflated)
    start_row = window_start[0]
    z_matrix = vectors_window.reshape(N, W)
    vectors_updated = jnp.dot(z_matrix, rotation, precision=highest).reshape(vectors_window.shape)
    strip_matrix = column_strip.reshape(N, W)
    turned = jnp.dot(strip_matrix, rotation, precision=highest)
    row_number = jnp.arange(N, dtype=jnp.int32)
    column_updated = jnp.where(row_number[:, None] < start_row, turned, strip_matrix).reshape(column_strip.shape)
    row_panel = row_strip.reshape(W, N)
    rotated_rows = lax.dot_general(rotation, row_panel, (((0,), (0,)), ((), ())), precision=highest)
    column_number = jnp.arange(N, dtype=jnp.int32)
    row_updated = jnp.where(column_number[None, :] >= start_row + W, rotated_rows, row_panel).reshape(row_strip.shape)
    return (vectors_updated, column_updated, row_updated)
```

```python
import functools

import jax
import jax.numpy as jnp
from jax import lax
from jax.experimental import pallas as pl
from jax.experimental.pallas import tpu as pltpu
from jax.sharding import PartitionSpec as P

W = 1024
Z = 8
ROWS = 32
CHUNK = 64
MESH = pl.DeviceIdType.MESH


def send(src, dst, sent, landed, device):
    pltpu.make_async_remote_copy(
        src_ref=src, dst_ref=dst, send_sem=sent, recv_sem=landed, device_id=device, device_id_type=MESH
    ).start()


def drain(ref, semaphore):
    pltpu.make_async_copy(ref, ref, semaphore).wait()


def lanes(index, size=128):
    return pl.ds(pl.multiple_of(index * size, size), size)


def row_of(y, x, core):
    return (y * 4 + x) * 2 + core


def rotate(x, high, low, store):
    rows = x.shape[0]
    x_high = x.astype(jnp.bfloat16)
    x_low = (x - x_high.astype(jnp.float32)).astype(jnp.bfloat16)
    both = jnp.concatenate([x_high, x_low], axis=0)
    for n in range(4):
        columns = slice(256 * n, 256 * n + 256)
        top = jnp.dot(both, high[:, columns], preferred_element_type=jnp.float32)
        bottom = jnp.dot(x_high, low[:, columns], preferred_element_type=jnp.float32)
        store(columns, top[:rows] + top[rows:] + bottom)


def kernel(
    chunks, per_device, first_round,
    deflated, f_ref, z_ref, c_ref, s_ref,
    zo_ref, co_ref, so_ref,
    factor, high, low, z_in, c_in, z_out, c_out, s_in, s_out, s_turned, s_rotated,
    local, f_sent, f_landed, ring_sent, ring_landed, far_sent, far_landed, pair_sent, pair_landed,
    in_sent, z_landed, c_landed, out_sent, zo_landed, co_landed, s_sent, s_landed, so_sent, so_landed,
):
    row = lax.axis_index("row")
    mine = lax.axis_index("col")
    y, x, core = row // 8, (row // 2) % 4, row % 2
    barrier = pltpu.get_barrier_semaphore()

    @pl.loop(1, Z)
    def _(d):
        pl.semaphore_signal(barrier, inc=1, device_id=(row, (mine + d) % Z), device_id_type=MESH)

    @pl.loop(1, ROWS)
    def _(d):
        pl.semaphore_signal(barrier, inc=1, device_id=((row + d) % ROWS, mine), device_id_type=MESH)

    own = [
        pltpu.make_async_copy(f_ref, factor.at[y, x, core, :, lanes(mine)], local.at[0]),
        pltpu.make_async_copy(z_ref.at[:, mine], z_in.at[:, :, lanes(mine)], local.at[1]),
        pltpu.make_async_copy(c_ref.at[0:chunks, mine], c_in.at[0:chunks, :, lanes(mine)], local.at[2]),
    ]
    for copy in own:
        copy.start()
    pl.semaphore_wait(barrier, Z - 1 + ROWS - 1)

    far_first = (4, 3, 5, 2, 6, 1, 7)
    for d in far_first:
        peer = (row, (mine + d) % Z)
        send(f_ref, factor.at[y, x, core, :, lanes(mine)], f_sent, f_landed, peer)
    for d in far_first:
        other = (mine + d) % Z
        send(z_ref.at[:, other], z_in.at[:, :, lanes(mine)], in_sent.at[0], z_landed, (row, other))
    for d in far_first:
        other = (mine + d) % Z
        send(
            c_ref.at[0:chunks, other], c_in.at[0:chunks, :, lanes(mine)],
            in_sent.at[1], c_landed, (row, other),
        )

    own[0].wait()
    drain(factor.at[0, 0, 0, :, 0:896], f_landed)
    left, right = slice(0, 512), slice(512, 1024)
    for d in (2, 1, 3):
        piece = factor.at[y, x, core, :, left]
        send(piece, piece, ring_sent.at[0], ring_landed.at[0], (row_of(y, (x + d) % 4, core), mine))
        piece = factor.at[y, x, core, :, right]
        send(piece, piece, ring_sent.at[1], ring_landed.at[1], (row_of((y + d) % 4, x, core), mine))
    drain(factor.at[0, 0:3, 0, :, left], ring_landed.at[0])
    line_x = factor.at[y, :, core, :, left]
    for d in (2, 1, 3):
        send(line_x, line_x, far_sent.at[0], far_landed.at[0, d], (row_of((y + d) % 4, x, core), mine))
    drain(factor.at[0:3, 0, 0, :, right], ring_landed.at[1])
    line_y = factor.at[:, x, core, :, right]
    for d in (2, 1, 3):
        send(line_y, line_y, far_sent.at[1], far_landed.at[1, d], (row_of(y, (x + d) % 4, core), mine))

    partner = (row_of(y, x, 1 - core), mine)
    send(line_x, line_x, pair_sent, pair_landed, partner)
    send(line_y, line_y, pair_sent, pair_landed, partner)

    @pl.loop(1, ROWS)
    def _(d):
        other = (row + d) % ROWS
        for e in range(per_device):
            send(
                s_ref.at[:, first_round + other * per_device + e],
                s_in.at[e, pl.ds(row * 32, 32)],
                s_sent, s_landed, (other, mine),
            )

    own_rounds = [
        pltpu.make_async_copy(
            s_ref.at[:, first_round + row * per_device + e], s_in.at[e, pl.ds(row * 32, 32)], local.at[3 + e]
        )
        for e in range(per_device)
    ]
    for copy in own_rounds:
        copy.start()

    for d in (1, 3, 2):
        piece = factor.at[(y + 4 - d) % 4, :, core, :, left]
        drain(piece, far_landed.at[0, d])
        send(piece, piece, pair_sent, pair_landed, partner)
        piece = factor.at[:, (x + 4 - d) % 4, core, :, right]
        drain(piece, far_landed.at[1, d])
        send(piece, piece, pair_sent, pair_landed, partner)
    drain(factor.at[:, :, 0], pair_landed)

    spike = factor[0, 0, 0, 0:1, :]
    columns = lax.broadcasted_iota(jnp.int32, (1, W), 1)
    spike_row = jnp.where(columns < W - deflated[0], spike, 0.0)
    squares = jnp.sum(spike_row * spike_row, axis=1, keepdims=True)
    corner = spike[:, 0:1]
    magnitude = jnp.sqrt(squares + 1e-06)
    signum = jnp.where(corner >= 0, 1.0, -1.0)
    vector = spike_row + jnp.where(columns == 0, signum * magnitude, 0.0)
    denominator = squares + 2.0 * jnp.abs(corner) * magnitude + magnitude * magnitude
    scaling = 2.0 / denominator

    @pl.loop(0, ROWS)
    def _(b):
        block = factor[b // 8, (b // 2) % 4, b % 2]
        image = jnp.sum(block * vector, axis=1, keepdims=True)
        turned = block - (scaling * image) * vector
        top = turned.astype(jnp.bfloat16)
        high[pl.ds(pl.multiple_of(b * 32, 32), 32), :] = top
        low[pl.ds(pl.multiple_of(b * 32, 32), 32), :] = (turned - top.astype(jnp.float32)).astype(jnp.bfloat16)

    def turn(count, source, result, target, sent, landed):
        @pl.loop(0, count)
        def _(c):
            def store(columns, value):
                result[c, :, columns] = value

            rotate(source[c], high, low, store)
            for d in far_first:
                other = (mine + d) % Z
                send(result.at[c, :, lanes(other)], target.at[c, mine], sent, landed, (row, other))
            pltpu.make_async_copy(result.at[c, :, lanes(mine)], target.at[c, mine], local.at[5]).start()

    own[1].wait()
    drain(z_in.at[:, :, 0:896], z_landed)
    turn(4, z_in, z_out, zo_ref, out_sent.at[0], zo_landed)
    drain(z_out.at[:, :, 0:128], local.at[5])

    drain(s_in.at[0:per_device, 0:992], s_landed)
    for copy in own_rounds:
        copy.wait()
    for e in range(per_device):
        @pl.loop(0, 8)
        def _(k):
            s_turned[:, lanes(k)] = s_in[e, pl.ds(pl.multiple_of(k * 128, 128), 128), 0, :].T

        def store(columns, value):
            s_rotated[:, columns] = value

        rotate(s_turned[...], high, low, store)

        @pl.loop(0, 8)
        def _(k):
            s_out[e, pl.ds(pl.multiple_of(k * 128, 128), 128), 0, :] = s_rotated[:, lanes(k)].T

    @pl.loop(1, ROWS)
    def _(d):
        other = (row + d) % ROWS
        for e in range(per_device):
            send(
                s_out.at[e, pl.ds(other * 32, 32)],
                so_ref.at[:, first_round + row * per_device + e],
                so_sent, so_landed, (other, mine),
            )

    own_results = [
        pltpu.make_async_copy(
            s_out.at[e, pl.ds(row * 32, 32)], so_ref.at[:, first_round + row * per_device + e], local.at[6 + e]
        )
        for e in range(per_device)
    ]
    for copy in own_results:
        copy.start()

    own[2].wait()
    drain(c_in.at[0:chunks, :, 0:896], c_landed)
    turn(chunks, c_in, c_out, co_ref, out_sent.at[1], co_landed)
    drain(c_out.at[0:chunks, :, 0:128], local.at[5])

    for copy in own_results:
        copy.wait()
    drain(factor.at[0, 0, 0, :, 0:896], f_sent)
    for side in range(2):
        drain(factor.at[0, 0:3, 0, :, left], ring_sent.at[side])
        drain(factor.at[0:3, :, 0, :, left], far_sent.at[side])
    drain(factor.at[:, :, 0], pair_sent)
    drain(z_in.at[:, :, 0:896], in_sent.at[0])
    drain(c_in.at[0:chunks, :, 0:896], in_sent.at[1])
    drain(s_in.at[0:per_device, 0:992], s_sent)
    drain(s_in.at[0:per_device, 0:992], so_sent)
    drain(s_in.at[0:per_device, 0:992], so_landed)
    drain(z_out.at[:, :, 0:896], out_sent.at[0])
    drain(c_out.at[0:chunks, :, 0:896], out_sent.at[1])
    drain(z_out.at[:, :, 0:896], zo_landed)
    drain(c_out.at[0:chunks, :, 0:896], co_landed)


def variant(chunks):
    per_device, first_round = (2, 0) if chunks <= 2 else (1, 32)
    anywhere = pl.BlockSpec(memory_space=pl.ANY)
    blocks = jax.ShapeDtypeStruct((4, Z, CHUNK, 128), jnp.float32)
    dma = pltpu.SemaphoreType.DMA
    return pl.pallas_call(
        functools.partial(kernel, chunks, per_device, first_round),
        name=f"window_{chunks}",
        out_shape=(blocks, blocks, jax.ShapeDtypeStruct((32, 64, 1, 128), jnp.float32)),
        in_specs=[
            pl.BlockSpec(memory_space=pltpu.SMEM), pl.BlockSpec(memory_space=pltpu.VMEM),
            anywhere, anywhere, anywhere,
        ],
        out_specs=(anywhere, anywhere, anywhere),
        scratch_shapes=[
            pltpu.VMEM((4, 4, 2, 32, W), jnp.float32),
            pltpu.VMEM((W, W), jnp.bfloat16),
            pltpu.VMEM((W, W), jnp.bfloat16),
            *[pltpu.VMEM((4, CHUNK, W), jnp.float32) for _ in range(4)],
            *[pltpu.VMEM((2, W, 1, 128), jnp.float32) for _ in range(2)],
            *[pltpu.VMEM((128, W), jnp.float32) for _ in range(2)],
            dma((8,)),
            dma, dma, dma((2,)), dma((2,)), dma((2,)), dma((2, 4)), dma, dma,
            dma((2,)), dma, dma, dma((2,)), dma, dma, dma, dma, dma, dma,
        ],
        compiler_params=pltpu.CompilerParams(
            collective_id=chunks, has_side_effects=True, vmem_limit_bytes=48 * 1024 * 1024
        ),
    )


def body(vectors_window, column_strip, row_strip, factor, window_start, deflated):
    start = window_start[0]
    strip_blocks = column_strip.reshape(4, Z, CHUNK, 128)
    operands = (deflated, factor, vectors_window.reshape(4, Z, CHUNK, 128), strip_blocks, row_strip)
    vectors, strip, rows = lax.switch(
        (start - 1) // 16384, [variant(chunks) for chunks in (1, 2, 3, 4)], *operands
    )
    shape = (32, 1, 64, 128)
    row_number = (
        (lax.broadcasted_iota(jnp.int32, shape, 0) * ROWS + lax.axis_index("row")) * 64
        + lax.broadcasted_iota(jnp.int32, shape, 2)
    )
    column_updated = jnp.where(row_number < start, strip.reshape(shape), column_strip)
    column_number = (
        (lax.broadcasted_iota(jnp.int32, row_strip.shape, 1) * Z + lax.axis_index("col")) * 128
        + lax.broadcasted_iota(jnp.int32, row_strip.shape, 3)
    )
    row_updated = jnp.where(column_number >= start + W, rows, row_strip)
    return vectors.reshape(shape), column_updated, row_updated


def solution(mesh):
    return jax.shard_map(
        body,
        mesh=mesh,
        in_specs=(
            P(None, "row", None, "col"),
            P(None, "row", None, "col"),
            P("row", None, "col", None),
            P("row", "col"),
            P(),
            P(),
        ),
        out_specs=(
            P(None, "row", None, "col"),
            P(None, "row", None, "col"),
            P("row", None, "col", None),
        ),
        check_vma=False,
    )
```

```python
import functools

import jax
import jax.numpy as jnp
from jax import lax
from jax.experimental import pallas as pl
from jax.experimental.pallas import tpu as pltpu
from jax.sharding import PartitionSpec as P

W = 1024
Z = 8
ROWS = 32
ROUNDS = 32
STEP = 4
MESH = pl.DeviceIdType.MESH


def send(src, dst, sent, landed, device):
    pltpu.make_async_remote_copy(
        src_ref=src, dst_ref=dst, send_sem=sent, recv_sem=landed, device_id=device, device_id_type=MESH
    ).start()


def drain(ref, semaphore):
    pltpu.make_async_copy(ref, ref, semaphore).wait()


def lanes(index, size=128):
    return pl.ds(pl.multiple_of(index * size, size), size)


def row_of(y, x, core):
    return (y * 4 + x) * 2 + core


def rotate(x, high, low, store):
    rows = x.shape[0]
    x_high = x.astype(jnp.bfloat16)
    x_low = (x - x_high.astype(jnp.float32)).astype(jnp.bfloat16)
    both = jnp.concatenate([x_high, x_low], axis=0)
    for n in range(4):
        columns = slice(256 * n, 256 * n + 256)
        top = jnp.dot(both, high[:, columns], preferred_element_type=jnp.float32)
        bottom = jnp.dot(x_high, low[:, columns], preferred_element_type=jnp.float32)
        store(columns, top[:rows] + top[rows:] + bottom)


def kernel(
    rounds, per_device, first_round,
    starts, deflated, f_ref, z_ref, c_ref, s_ref,
    zo_ref, co_ref, so_ref,
    factor, high, low, z_in, c_in, z_out, c_out, s_in, s_out, s_turned, s_rotated,
    local, f_sent, f_landed, ring_sent, ring_landed, far_sent, far_landed, pair_sent, pair_landed,
    in_sent, z_landed, c_landed, out_sent, zo_landed, co_landed, s_sent, s_landed, so_sent, so_landed,
):
    row = lax.axis_index("row")
    mine = lax.axis_index("col")
    y, x, core = row // 8, (row // 2) % 4, row % 2
    barrier = pltpu.get_barrier_semaphore()
    own_factor = factor.at[y, x, core, :, lanes(mine)]
    load = pltpu.make_async_copy(f_ref, own_factor, local.at[0])
    load.start()

    @pl.loop(1, Z)
    def _(d):
        pl.semaphore_signal(barrier, inc=1, device_id=(row, (mine + d) % Z), device_id_type=MESH)

    @pl.loop(1, ROWS)
    def _(d):
        pl.semaphore_signal(barrier, inc=1, device_id=((row + d) % ROWS, mine), device_id_type=MESH)

    start = starts[0]
    untouched = []
    if rounds < ROUNDS:
        untouched.append((c_ref.at[rounds:], co_ref.at[rounds:]))
    if first_round:
        untouched.append((s_ref.at[:, 0:first_round], so_ref.at[:, 0:first_round]))
    own = [
        pltpu.make_async_copy(z_ref.at[:, mine], z_in.at[:, :, lanes(mine)], local.at[1]),
        pltpu.make_async_copy(c_ref.at[0:rounds, mine], c_in.at[0:rounds, :, lanes(mine)], local.at[2]),
    ]
    for copy in own:
        copy.start()
    kept = [pltpu.make_async_copy(source, target, local.at[8 + n]) for n, (source, target) in enumerate(untouched)]
    load.wait()
    pl.semaphore_wait(barrier, Z - 1 + ROWS - 1)

    far_first = (4, 3, 5, 2, 6, 1, 7)
    for d in far_first:
        send(own_factor, own_factor, f_sent, f_landed, (row, (mine + d) % Z))
    for d in far_first:
        other = (mine + d) % Z
        send(z_ref.at[:, other], z_in.at[:, :, lanes(mine)], in_sent.at[0], z_landed, (row, other))
    for copy in kept:
        copy.start()
    for d in far_first:
        other = (mine + d) % Z
        send(
            c_ref.at[0:rounds, other], c_in.at[0:rounds, :, lanes(mine)],
            in_sent.at[1], c_landed, (row, other),
        )

    left, right = slice(0, 512), slice(512, 1024)
    partner = (row_of(y, x, 1 - core), mine)

    def along_x(d):
        return row_of(y, (x + d) % 4, core), mine

    def along_y(d):
        return row_of((y + d) % 4, x, core), mine

    drain(factor.at[0, 0, 0, :, 0:896], f_landed)
    piece_left, piece_right = factor.at[y, x, core, :, left], factor.at[y, x, core, :, right]
    for d in (2, 1, 3):
        send(piece_left, piece_left, ring_sent.at[0], ring_landed.at[0, d], along_x(d))
        send(piece_right, piece_right, ring_sent.at[1], ring_landed.at[1, d], along_y(d))
    for d in (2, 1, 3):
        send(piece_left, piece_left, far_sent.at[0], far_landed.at[0, d], along_y(d))
        send(piece_right, piece_right, far_sent.at[1], far_landed.at[1, d], along_x(d))
    send(piece_left, piece_left, pair_sent, pair_landed, partner)
    send(piece_right, piece_right, pair_sent, pair_landed, partner)
    for e in (1, 3, 2):
        piece_left = factor.at[y, (x + 4 - e) % 4, core, :, left]
        drain(piece_left, ring_landed.at[0, e])
        for d in (2, 1, 3):
            send(piece_left, piece_left, far_sent.at[0], far_landed.at[0, d], along_y(d))
        piece_right = factor.at[(y + 4 - e) % 4, x, core, :, right]
        drain(piece_right, ring_landed.at[1, e])
        for d in (2, 1, 3):
            send(piece_right, piece_right, far_sent.at[1], far_landed.at[1, d], along_x(d))
        send(piece_left, piece_left, pair_sent, pair_landed, partner)
        send(piece_right, piece_right, pair_sent, pair_landed, partner)

    @pl.loop(1, ROWS)
    def _(d):
        other = (row + d) % ROWS
        for e in range(per_device):
            send(
                s_ref.at[:, first_round + other * per_device + e],
                s_in.at[e, pl.ds(row * 32, 32)],
                s_sent, s_landed, (other, mine),
            )

    own_rounds = [
        pltpu.make_async_copy(
            s_ref.at[:, first_round + row * per_device + e], s_in.at[e, pl.ds(row * 32, 32)], local.at[3 + e]
        )
        for e in range(per_device)
    ]
    for copy in own_rounds:
        copy.start()

    for d in (1, 3, 2):
        line = factor.at[(y + 4 - d) % 4, :, core, :, left]
        drain(line, far_landed.at[0, d])
        send(line, line, pair_sent, pair_landed, partner)
        line = factor.at[:, (x + 4 - d) % 4, core, :, right]
        drain(line, far_landed.at[1, d])
        send(line, line, pair_sent, pair_landed, partner)
    drain(factor.at[:, :, 0], pair_landed)

    spike = factor[0, 0, 0, 0:1, :]
    columns = lax.broadcasted_iota(jnp.int32, (1, W), 1)
    spike_row = jnp.where(columns < W - deflated[0], spike, 0.0)
    squares = jnp.sum(spike_row * spike_row, axis=1, keepdims=True)
    corner = spike[:, 0:1]
    magnitude = jnp.sqrt(squares + 1e-06)
    signum = jnp.where(corner >= 0, 1.0, -1.0)
    vector = spike_row + jnp.where(columns == 0, signum * magnitude, 0.0)
    denominator = squares + 2.0 * jnp.abs(corner) * magnitude + magnitude * magnitude
    scaling = 2.0 / denominator

    @pl.loop(0, ROWS, unroll=4)
    def _(b):
        block = factor[b // 8, (b // 2) % 4, b % 2]
        image = jnp.sum(block * vector, axis=1, keepdims=True)
        turned = block - (scaling * image) * vector
        top = turned.astype(jnp.bfloat16)
        high[pl.ds(pl.multiple_of(b * 32, 32), 32), :] = top
        low[pl.ds(pl.multiple_of(b * 32, 32), 32), :] = (turned - top.astype(jnp.float32)).astype(jnp.bfloat16)

    def turn_some(first, count, source, result, target, sent, landed, bounded):
        some = pl.ds(first, count)
        shape = (count, 8, 256)
        number = (
            ((first + lax.broadcasted_iota(jnp.int32, shape, 0)) * ROWS + row) * 64
            + mine * 8 + lax.broadcasted_iota(jnp.int32, shape, 1)
        )

        def store(columns, value):
            value = value.reshape(shape)
            if bounded:
                value = jnp.where(number < start, value, source[some, :, columns])
            result[some, :, columns] = value

        rotate(source[some].reshape(count * 8, W), high, low, store)
        for d in far_first:
            other = (mine + d) % Z
            send(result.at[some, :, lanes(other)], target.at[some, mine], sent, landed, (row, other))
        pltpu.make_async_copy(result.at[some, :, lanes(mine)], target.at[some, mine], local.at[5]).start()

    def turn(count, *where):
        if count >= 8:
            @pl.loop(0, count // 8)
            def _(c):
                turn_some(pl.multiple_of(c * 8, 8), 8, *where)

        if count % 8:
            turn_some(count - count % 8, count % 8, *where)

    own[0].wait()
    drain(z_in.at[:, :, 0:896], z_landed)
    turn(ROUNDS, z_in, z_out, zo_ref, out_sent.at[0], zo_landed, False)
    drain(z_out.at[:, :, 0:128], local.at[5])

    drain(s_in.at[0:per_device, 0:992], s_landed)
    for copy in own_rounds:
        copy.wait()
    for e in range(per_device):
        @pl.loop(0, 8)
        def _(k):
            s_turned[:, lanes(k)] = s_in[e, pl.ds(pl.multiple_of(k * 128, 128), 128), 0, :].T

        number = (
            ((first_round + row * per_device + e) * Z + mine) * 128
            + lax.broadcasted_iota(jnp.int32, (128, 256), 0)
        )

        def store(columns, value):
            s_rotated[:, columns] = jnp.where(number >= start + W, value, s_turned[:, columns])

        rotate(s_turned[...], high, low, store)

        @pl.loop(0, 8)
        def _(k):
            s_out[e, pl.ds(pl.multiple_of(k * 128, 128), 128), 0, :] = s_rotated[:, lanes(k)].T

    @pl.loop(1, ROWS)
    def _(d):
        other = (row + d) % ROWS
        for e in range(per_device):
            send(
                s_out.at[e, pl.ds(other * 32, 32)],
                so_ref.at[:, first_round + row * per_device + e],
                so_sent, so_landed, (other, mine),
            )

    own_results = [
        pltpu.make_async_copy(
            s_out.at[e, pl.ds(row * 32, 32)], so_ref.at[:, first_round + row * per_device + e], local.at[6 + e]
        )
        for e in range(per_device)
    ]
    for copy in own_results:
        copy.start()

    own[1].wait()
    drain(c_in.at[0:rounds, :, 0:896], c_landed)
    turn(rounds, c_in, c_out, co_ref, out_sent.at[1], co_landed, True)
    drain(c_out.at[0:rounds, :, 0:128], local.at[5])

    for copy in own_results + kept:
        copy.wait()
    drain(factor.at[0, 0, 0, :, 0:896], f_sent)
    for side in range(2):
        drain(factor.at[0, 0:3, 0, :, left], ring_sent.at[side])
        drain(factor.at[0:3, :, 0, :, left], far_sent.at[side])
    drain(factor.at[:, :, 0], pair_sent)
    drain(z_in.at[:, :, 0:896], in_sent.at[0])
    drain(c_in.at[0:rounds, :, 0:896], in_sent.at[1])
    drain(s_in.at[0:per_device, 0:992], s_sent)
    drain(s_in.at[0:per_device, 0:992], so_sent)
    drain(s_in.at[0:per_device, 0:992], so_landed)
    drain(z_out.at[:, :, 0:896], out_sent.at[0])
    drain(c_out.at[0:rounds, :, 0:896], out_sent.at[1])
    drain(z_out.at[:, :, 0:896], zo_landed)
    drain(c_out.at[0:rounds, :, 0:896], co_landed)


def variant(rounds):
    per_device, first_round = (2, 0) if rounds <= 16 else (1, 32)
    anywhere = pl.BlockSpec(memory_space=pl.ANY)
    blocks = jax.ShapeDtypeStruct((ROUNDS, Z, 8, 128), jnp.float32)
    dma = pltpu.SemaphoreType.DMA
    return pl.pallas_call(
        functools.partial(kernel, rounds, per_device, first_round),
        name=f"window_{rounds}",
        out_shape=(blocks, blocks, jax.ShapeDtypeStruct((32, 64, 1, 128), jnp.float32)),
        in_specs=[*[pl.BlockSpec(memory_space=pltpu.SMEM)] * 2, *[pl.BlockSpec(memory_space=pltpu.HBM)] * 4],
        out_specs=(anywhere, anywhere, anywhere),
        scratch_shapes=[
            pltpu.VMEM((4, 4, 2, 32, W), jnp.float32),
            pltpu.VMEM((W, W), jnp.bfloat16),
            pltpu.VMEM((W, W), jnp.bfloat16),
            *[pltpu.VMEM((ROUNDS, 8, W), jnp.float32) for _ in range(4)],
            *[pltpu.VMEM((2, W, 1, 128), jnp.float32) for _ in range(2)],
            *[pltpu.VMEM((128, W), jnp.float32) for _ in range(2)],
            dma((10,)),
            dma, dma, dma((2,)), dma((2, 4)), dma((2,)), dma((2, 4)), dma, dma,
            dma((2,)), dma, dma, dma((2,)), dma, dma, dma, dma, dma, dma,
        ],
        compiler_params=pltpu.CompilerParams(
            collective_id=rounds // STEP, has_side_effects=True, vmem_limit_bytes=48 * 1024 * 1024
        ),
    )


def body(vectors_window, column_strip, row_strip, factor, window_start, deflated):
    start = window_start[0]
    by_worker = (ROUNDS, Z, 8, 128)
    vectors, strip, rows = lax.switch(
        (start - 1) // (64 * ROWS * STEP),
        [variant(rounds) for rounds in range(STEP, ROUNDS + 1, STEP)],
        window_start, deflated, factor,
        vectors_window.reshape(by_worker), column_strip.reshape(by_worker), row_strip,
    )
    return vectors.reshape(vectors_window.shape), strip.reshape(column_strip.shape), rows


def solution(mesh):
    return jax.shard_map(
        body,
        mesh=mesh,
        in_specs=(
            P(None, "row", None, "col"),
            P(None, "row", None, "col"),
            P("row", None, "col", None),
            P("row", "col"),
            P(),
            P(),
        ),
        out_specs=(
            P(None, "row", None, "col"),
            P(None, "row", None, "col"),
            P("row", None, "col", None),
        ),
        check_vma=False,
    )
```

```python
import functools

import jax
import jax.numpy as jnp
from jax import lax
from jax.experimental import pallas as pl
from jax.experimental.pallas import tpu as pltpu
from jax.sharding import PartitionSpec as P

W = 1024
Z = 8
ROWS = 32
ROUNDS = 32
STEP = 2
MESH = pl.DeviceIdType.MESH


def send(src, dst, sent, landed, device):
    pltpu.make_async_remote_copy(
        src_ref=src, dst_ref=dst, send_sem=sent, recv_sem=landed, device_id=device, device_id_type=MESH
    ).start()


def drain(ref, semaphore):
    pltpu.make_async_copy(ref, ref, semaphore).wait()


def lanes(index, size=128):
    return pl.ds(pl.multiple_of(index * size, size), size)


def row_of(y, x, core):
    return (y * 4 + x) * 2 + core


def rotate(x, high, low, store):
    rows = x.shape[0]
    x_high = x.astype(jnp.bfloat16)
    x_low = (x - x_high.astype(jnp.float32)).astype(jnp.bfloat16)
    both = jnp.concatenate([x_high, x_low], axis=0)

    @pl.loop(0, 4, unroll=1)
    def _(n):
        columns = lanes(n, 256)
        top = jnp.dot(both, high[:, columns], preferred_element_type=jnp.float32)
        bottom = jnp.dot(x_high, low[:, columns], preferred_element_type=jnp.float32)
        store(columns, top[:rows] + top[rows:] + bottom)


def kernel(
    rounds, per_device, first_round,
    starts, deflated, f_ref, z_ref, c_ref, s_ref,
    zo_ref, co_ref, so_ref,
    factor, high, low, x_in, x_out, s_in, s_out, s_turned, s_rotated,
    local, f_sent, f_landed, ring_sent, ring_landed, far_sent, far_landed, pair_sent, pair_landed,
    in_sent, in_landed, out_sent, out_landed, s_sent, s_landed, so_sent, so_landed,
):
    row = lax.axis_index("row")
    mine = lax.axis_index("col")
    y, x, core = row // 8, (row // 2) % 4, row % 2
    barrier = pltpu.get_barrier_semaphore()
    own_factor = factor.at[y, x, core, :, lanes(mine)]
    load = pltpu.make_async_copy(f_ref, own_factor, local.at[0])
    load.start()

    @pl.loop(1, Z)
    def _(d):
        pl.semaphore_signal(barrier, inc=1, device_id=(row, (mine + d) % Z), device_id_type=MESH)

    @pl.loop(1, ROWS)
    def _(d):
        pl.semaphore_signal(barrier, inc=1, device_id=((row + d) % ROWS, mine), device_id_type=MESH)

    start = starts[0]
    total = ROUNDS + rounds
    untouched = []
    if rounds < ROUNDS:
        untouched.append((c_ref.at[rounds:], co_ref.at[rounds:]))
    if first_round:
        untouched.append((s_ref.at[:, 0:first_round], so_ref.at[:, 0:first_round]))
    own = [
        pltpu.make_async_copy(z_ref.at[:, mine], x_in.at[0:ROUNDS, :, lanes(mine)], local.at[1]),
        pltpu.make_async_copy(c_ref.at[0:rounds, mine], x_in.at[ROUNDS:total, :, lanes(mine)], local.at[2]),
    ]
    for copy in own:
        copy.start()
    kept = [pltpu.make_async_copy(source, target, local.at[8 + n]) for n, (source, target) in enumerate(untouched)]
    load.wait()
    pl.semaphore_wait(barrier, Z - 1 + ROWS - 1)

    def over_z(move):
        @pl.loop(0, Z - 1)
        def _(i):
            move((mine + 4 + (1 - 2 * (i % 2)) * ((i + 1) // 2)) % Z)

    over_z(lambda other: send(own_factor, own_factor, f_sent, f_landed, (row, other)))
    over_z(lambda other: send(
        z_ref.at[:, other], x_in.at[0:ROUNDS, :, lanes(mine)], in_sent.at[0], in_landed.at[0], (row, other)
    ))
    over_z(lambda other: send(
        c_ref.at[0:rounds, other], x_in.at[ROUNDS:total, :, lanes(mine)],
        in_sent.at[1], in_landed.at[1], (row, other),
    ))

    left, right = slice(0, 512), slice(512, 1024)
    partner = (row_of(y, x, 1 - core), mine)

    def along_x(d):
        return row_of(y, (x + d) % 4, core), mine

    def along_y(d):
        return row_of((y + d) % 4, x, core), mine

    def forward(piece, side, across):
        @pl.loop(0, 3)
        def _(i):
            d = (i + 1) % 3 + 1
            send(piece, piece, far_sent.at[side], far_landed.at[side, d], across(d))

    drain(factor.at[0, 0, 0, :, 0:896], f_landed)
    piece_left, piece_right = factor.at[y, x, core, :, left], factor.at[y, x, core, :, right]

    @pl.loop(0, 3)
    def _(i):
        d = (i + 1) % 3 + 1
        send(piece_left, piece_left, ring_sent.at[0], ring_landed.at[0, d], along_x(d))
        send(piece_right, piece_right, ring_sent.at[1], ring_landed.at[1, d], along_y(d))

    forward(piece_left, 0, along_y)
    forward(piece_right, 1, along_x)
    send(piece_left, piece_left, pair_sent, pair_landed, partner)
    send(piece_right, piece_right, pair_sent, pair_landed, partner)

    @pl.loop(0, 3)
    def _(i):
        e = 1 + i * 2 - 3 * (i // 2)
        piece = factor.at[y, (x + 4 - e) % 4, core, :, left]
        drain(piece, ring_landed.at[0, e])
        forward(piece, 0, along_y)
        send(piece, piece, pair_sent, pair_landed, partner)
        piece = factor.at[(y + 4 - e) % 4, x, core, :, right]
        drain(piece, ring_landed.at[1, e])
        forward(piece, 1, along_x)
        send(piece, piece, pair_sent, pair_landed, partner)

    @pl.loop(1, ROWS)
    def _(d):
        other = (row + d) % ROWS
        for e in range(per_device):
            send(
                s_ref.at[:, first_round + other * per_device + e],
                s_in.at[e, pl.ds(row * 32, 32)],
                s_sent, s_landed, (other, mine),
            )

    own_rounds = [
        pltpu.make_async_copy(
            s_ref.at[:, first_round + row * per_device + e], s_in.at[e, pl.ds(row * 32, 32)], local.at[3 + e]
        )
        for e in range(per_device)
    ]
    for copy in own_rounds + kept:
        copy.start()

    @pl.loop(0, 3)
    def _(i):
        d = 1 + i * 2 - 3 * (i // 2)
        line = factor.at[(y + 4 - d) % 4, :, core, :, left]
        drain(line, far_landed.at[0, d])
        send(line, line, pair_sent, pair_landed, partner)
        line = factor.at[:, (x + 4 - d) % 4, core, :, right]
        drain(line, far_landed.at[1, d])
        send(line, line, pair_sent, pair_landed, partner)

    drain(factor.at[:, :, 0], pair_landed)

    spike = factor[0, 0, 0, 0:1, :]
    columns = lax.broadcasted_iota(jnp.int32, (1, W), 1)
    spike_row = jnp.where(columns < W - deflated[0], spike, 0.0)
    squares = jnp.sum(spike_row * spike_row, axis=1, keepdims=True)
    corner = spike[:, 0:1]
    magnitude = jnp.sqrt(squares + 1e-06)
    signum = jnp.where(corner >= 0, 1.0, -1.0)
    vector = spike_row + jnp.where(columns == 0, signum * magnitude, 0.0)
    denominator = squares + 2.0 * jnp.abs(corner) * magnitude + magnitude * magnitude
    scaling = 2.0 / denominator

    @pl.loop(0, ROWS, unroll=4)
    def _(b):
        block = factor[b // 8, (b // 2) % 4, b % 2]
        image = jnp.sum(block * vector, axis=1, keepdims=True)
        turned = block - (scaling * image) * vector
        top = turned.astype(jnp.bfloat16)
        high[pl.ds(pl.multiple_of(b * 32, 32), 32), :] = top
        low[pl.ds(pl.multiple_of(b * 32, 32), 32), :] = (turned - top.astype(jnp.float32)).astype(jnp.bfloat16)

    def turn(first, count):
        some = pl.ds(first, count)
        shape = (count, 8, 256)
        number = (
            ((first - ROUNDS + lax.broadcasted_iota(jnp.int32, shape, 0)) * ROWS + row) * 64
            + mine * 8 + lax.broadcasted_iota(jnp.int32, shape, 1)
        )

        def store(columns, value):
            x_out[some, :, columns] = jnp.where(number < start, value.reshape(shape), x_in[some, :, columns])

        rotate(x_in[some].reshape(count * 8, W), high, low, store)

        def give(target, base, side):
            where = pl.ds(first - base, count)
            over_z(lambda other: send(
                x_out.at[some, :, lanes(other)], target.at[where, mine],
                out_sent.at[side], out_landed.at[side], (row, other),
            ))
            pltpu.make_async_copy(x_out.at[some, :, lanes(mine)], target.at[where, mine], local.at[5]).start()

        if isinstance(first, int):
            give(co_ref, ROUNDS, 1)
        else:
            pl.when(first < ROUNDS)(lambda: give(zo_ref, 0, 0))
            pl.when(first >= ROUNDS)(lambda: give(co_ref, ROUNDS, 1))

    def turn_strip():
        drain(s_in.at[0:per_device, 0:992], s_landed)
        for copy in own_rounds:
            copy.wait()

        @pl.loop(0, per_device)
        def _(e):
            @pl.loop(0, 8)
            def _(k):
                s_turned[:, lanes(k)] = s_in[e, pl.ds(pl.multiple_of(k * 128, 128), 128), 0, :].T

            number = (
                ((first_round + row * per_device + e) * Z + mine) * 128
                + lax.broadcasted_iota(jnp.int32, (128, 256), 0)
            )

            def store(columns, value):
                s_rotated[:, columns] = jnp.where(number >= start + W, value, s_turned[:, columns])

            rotate(s_turned[...], high, low, store)

            @pl.loop(0, 8)
            def _(k):
                s_out[e, pl.ds(pl.multiple_of(k * 128, 128), 128), 0, :] = s_rotated[:, lanes(k)].T

        @pl.loop(1, ROWS)
        def _(d):
            other = (row + d) % ROWS
            for e in range(per_device):
                send(
                    s_out.at[e, pl.ds(other * 32, 32)],
                    so_ref.at[:, first_round + row * per_device + e],
                    so_sent, so_landed, (other, mine),
                )

        for copy in own_results:
            copy.start()
        own[1].wait()
        drain(x_in.at[ROUNDS:total, :, 0:896], in_landed.at[1])

    own_results = [
        pltpu.make_async_copy(
            s_out.at[e, pl.ds(row * 32, 32)], so_ref.at[:, first_round + row * per_device + e], local.at[6 + e]
        )
        for e in range(per_device)
    ]
    own[0].wait()
    drain(x_in.at[0:ROUNDS, :, 0:896], in_landed.at[0])

    @pl.loop(0, total // 8)
    def _(c):
        if rounds >= 8:
            pl.when(c == ROUNDS // 8)(turn_strip)
        turn(pl.multiple_of(c * 8, 8), 8)

    if rounds < 8:
        turn_strip()
    if total % 8:
        turn(total - total % 8, total % 8)
    drain(x_out.at[0:total, :, 0:128], local.at[5])

    for copy in own_results + kept:
        copy.wait()
    drain(factor.at[0, 0, 0, :, 0:896], f_sent)
    for side in range(2):
        drain(factor.at[0, 0:3, 0, :, left], ring_sent.at[side])
        drain(factor.at[0:3, :, 0, :, left], far_sent.at[side])
    drain(factor.at[:, :, 0], pair_sent)
    drain(s_in.at[0:per_device, 0:992], s_sent)
    drain(s_in.at[0:per_device, 0:992], so_sent)
    drain(s_in.at[0:per_device, 0:992], so_landed)
    for side, part in enumerate((slice(0, ROUNDS), slice(ROUNDS, total))):
        for semaphores in (in_sent, out_sent, out_landed):
            drain(x_in.at[part, :, 0:896], semaphores.at[side])


def variant(rounds):
    per_device, first_round = (2, 0) if rounds <= 16 else (1, 32)
    anywhere = pl.BlockSpec(memory_space=pl.ANY)
    blocks = jax.ShapeDtypeStruct((ROUNDS, Z, 8, 128), jnp.float32)
    dma = pltpu.SemaphoreType.DMA
    return pl.pallas_call(
        functools.partial(kernel, rounds, per_device, first_round),
        name=f"window_{rounds}",
        out_shape=(blocks, blocks, jax.ShapeDtypeStruct((32, 64, 1, 128), jnp.float32)),
        in_specs=[*[pl.BlockSpec(memory_space=pltpu.SMEM)] * 2, *[pl.BlockSpec(memory_space=pltpu.HBM)] * 4],
        out_specs=(anywhere, anywhere, anywhere),
        scratch_shapes=[
            pltpu.VMEM((4, 4, 2, 32, W), jnp.float32),
            pltpu.VMEM((W, W), jnp.bfloat16),
            pltpu.VMEM((W, W), jnp.bfloat16),
            *[pltpu.VMEM((2 * ROUNDS, 8, W), jnp.float32) for _ in range(2)],
            *[pltpu.VMEM((2, W, 1, 128), jnp.float32) for _ in range(2)],
            *[pltpu.VMEM((128, W), jnp.float32) for _ in range(2)],
            dma((10,)),
            dma, dma, dma((2,)), dma((2, 4)), dma((2,)), dma((2, 4)), dma, dma,
            dma((2,)), dma((2,)), dma((2,)), dma((2,)), dma, dma, dma, dma,
        ],
        compiler_params=pltpu.CompilerParams(
            collective_id=rounds // STEP, has_side_effects=True, vmem_limit_bytes=48 * 1024 * 1024
        ),
    )


def put_down(*arrays):
    def copies(*refs):
        sources, targets, semaphores = refs[: len(arrays)], refs[len(arrays): -1], refs[-1]
        moves = [
            pltpu.make_async_copy(source.at[pl.ds(8 * part, 8)], target.at[pl.ds(8 * part, 8)], semaphores.at[n, part])
            for n, (source, target) in enumerate(zip(sources, targets))
            for part in range(4)
        ]
        for move in moves:
            move.start()
        for move in moves:
            move.wait()

    anywhere = [pl.BlockSpec(memory_space=pl.ANY)] * len(arrays)
    return pl.pallas_call(
        copies,
        name="put_down",
        out_shape=tuple(jax.ShapeDtypeStruct(array.shape, array.dtype) for array in arrays),
        in_specs=anywhere,
        out_specs=anywhere,
        scratch_shapes=[pltpu.SemaphoreType.DMA((len(arrays), 4))],
    )(*arrays)


def body(vectors_window, column_strip, row_strip, factor, window_start, deflated):
    start = window_start[0]
    by_worker = (ROUNDS, Z, 8, 128)
    vectors, strip, rows = lax.switch(
        (start - 1) // (64 * ROWS * STEP),
        [variant(rounds) for rounds in range(STEP, ROUNDS + 1, STEP)],
        window_start, deflated, pltpu.with_memory_space_constraint(factor, pltpu.HBM),
        vectors_window.reshape(by_worker), column_strip.reshape(by_worker), row_strip,
    )
    vectors, strip, rows = put_down(vectors, strip, rows)
    return vectors.reshape(vectors_window.shape), strip.reshape(column_strip.shape), rows


def solution(mesh):
    return jax.shard_map(
        body,
        mesh=mesh,
        in_specs=(
            P(None, "row", None, "col"),
            P(None, "row", None, "col"),
            P("row", None, "col", None),
            P("row", "col"),
            P(),
            P(),
        ),
        out_specs=(
            P(None, "row", None, "col"),
            P(None, "row", None, "col"),
            P("row", None, "col", None),
        ),
        check_vma=False,
    )
```

```python
import functools

import jax
import jax.numpy as jnp
from jax import lax
from jax.experimental import pallas as pl
from jax.experimental.pallas import tpu as pltpu
from jax.sharding import PartitionSpec as P

W = 1024
Z = 8
ROWS = 32
ROUNDS = 32
STEP = 2
MESH = pl.DeviceIdType.MESH


def send(src, dst, sent, landed, device):
    pltpu.make_async_remote_copy(
        src_ref=src, dst_ref=dst, send_sem=sent, recv_sem=landed, device_id=device, device_id_type=MESH
    ).start()


def drain(ref, semaphore):
    pltpu.make_async_copy(ref, ref, semaphore).wait()


def lanes(index, size=128):
    return pl.ds(pl.multiple_of(index * size, size), size)


def row_of(y, x, core):
    return (y * 4 + x) * 2 + core


def rotate(x, high, low, store):
    rows = x.shape[0]
    x_high = x.astype(jnp.bfloat16)
    x_low = (x - x_high.astype(jnp.float32)).astype(jnp.bfloat16)
    both = jnp.concatenate([x_high, x_low], axis=0)

    @pl.loop(0, 4, unroll=1)
    def _(n):
        columns = lanes(n, 256)
        top = jnp.dot(both, high[:, columns], preferred_element_type=jnp.float32)
        bottom = jnp.dot(x_high, low[:, columns], preferred_element_type=jnp.float32)
        store(columns, top[:rows] + top[rows:] + bottom)


def kernel(
    rounds, per_device, first_round,
    starts, deflated, f_ref, z_ref, c_ref, s_ref,
    zo_ref, co_ref, so_ref,
    factor, high, low, x_in, x_out, s_in, s_out, s_turned, s_rotated,
    local, f_sent, f_landed, ring_sent, ring_landed, far_sent, far_landed, pair_sent, pair_landed,
    in_sent, in_landed, out_sent, out_landed, s_sent, s_landed, so_sent, so_landed,
):
    row = lax.axis_index("row")
    mine = lax.axis_index("col")
    y, x, core = row // 8, (row // 2) % 4, row % 2
    barrier = pltpu.get_barrier_semaphore()
    own_factor = factor.at[y, x, core, :, lanes(mine)]
    load = pltpu.make_async_copy(f_ref, own_factor, local.at[0])
    load.start()

    @pl.loop(1, Z)
    def _(d):
        pl.semaphore_signal(barrier, inc=1, device_id=(row, (mine + d) % Z), device_id_type=MESH)

    @pl.loop(1, ROWS)
    def _(d):
        pl.semaphore_signal(barrier, inc=1, device_id=((row + d) % ROWS, mine), device_id_type=MESH)

    start = starts[0]
    total = ROUNDS + rounds
    untouched = []
    if rounds < ROUNDS:
        untouched.append((c_ref.at[rounds:], co_ref.at[rounds:]))
    if first_round:
        untouched.append((s_ref.at[:, 0:first_round], so_ref.at[:, 0:first_round]))
    own = [
        pltpu.make_async_copy(z_ref.at[:, mine], x_in.at[0:ROUNDS, :, lanes(mine)], local.at[1]),
        pltpu.make_async_copy(c_ref.at[0:rounds, mine], x_in.at[ROUNDS:total, :, lanes(mine)], local.at[2]),
    ]
    for copy in own:
        copy.start()
    kept = [pltpu.make_async_copy(source, target, local.at[8 + n]) for n, (source, target) in enumerate(untouched)]
    load.wait()
    pl.semaphore_wait(barrier, Z - 1 + ROWS - 1)

    def over_z(move):
        @pl.loop(0, Z - 1)
        def _(i):
            move((mine + 4 + (1 - 2 * (i % 2)) * ((i + 1) // 2)) % Z)

    over_z(lambda other: send(own_factor, own_factor, f_sent, f_landed, (row, other)))
    over_z(lambda other: send(
        z_ref.at[:, other], x_in.at[0:ROUNDS, :, lanes(mine)], in_sent.at[0], in_landed.at[0], (row, other)
    ))
    own_rounds = [
        pltpu.make_async_copy(
            s_ref.at[:, first_round + row * per_device + e], s_in.at[e, pl.ds(row * 32, 32)], local.at[3 + e]
        )
        for e in range(per_device)
    ]

    def spread_strip(e):
        @pl.loop(1, ROWS)
        def _(d):
            other = (row + d) % ROWS
            send(
                s_ref.at[:, first_round + other * per_device + e],
                s_in.at[e, pl.ds(row * 32, 32)],
                s_sent, s_landed.at[e], (other, mine),
            )

        own_rounds[e].start()

    spread_strip(0)
    over_z(lambda other: send(
        c_ref.at[0:rounds, other], x_in.at[ROUNDS:total, :, lanes(mine)],
        in_sent.at[1], in_landed.at[1], (row, other),
    ))

    left, right = slice(0, 512), slice(512, 1024)
    partner = (row_of(y, x, 1 - core), mine)

    def along_x(d):
        return row_of(y, (x + d) % 4, core), mine

    def along_y(d):
        return row_of((y + d) % 4, x, core), mine

    def forward(piece, side, across):
        @pl.loop(0, 3)
        def _(i):
            d = (i + 1) % 3 + 1
            send(piece, piece, far_sent.at[side], far_landed.at[side, d], across(d))

    drain(factor.at[0, 0, 0, :, 0:896], f_landed)
    piece_left, piece_right = factor.at[y, x, core, :, left], factor.at[y, x, core, :, right]

    @pl.loop(0, 3)
    def _(i):
        d = (i + 1) % 3 + 1
        send(piece_left, piece_left, ring_sent.at[0], ring_landed.at[0, d], along_x(d))
        send(piece_right, piece_right, ring_sent.at[1], ring_landed.at[1, d], along_y(d))

    forward(piece_left, 0, along_y)
    forward(piece_right, 1, along_x)
    send(piece_left, piece_left, pair_sent, pair_landed, partner)
    send(piece_right, piece_right, pair_sent, pair_landed, partner)

    @pl.loop(0, 3)
    def _(i):
        e = 1 + i * 2 - 3 * (i // 2)
        piece = factor.at[y, (x + 4 - e) % 4, core, :, left]
        drain(piece, ring_landed.at[0, e])
        forward(piece, 0, along_y)
        send(piece, piece, pair_sent, pair_landed, partner)
        piece = factor.at[(y + 4 - e) % 4, x, core, :, right]
        drain(piece, ring_landed.at[1, e])
        forward(piece, 1, along_x)
        send(piece, piece, pair_sent, pair_landed, partner)

    @pl.loop(0, 3)
    def _(i):
        d = 1 + i * 2 - 3 * (i // 2)
        line = factor.at[(y + 4 - d) % 4, :, core, :, left]
        drain(line, far_landed.at[0, d])
        send(line, line, pair_sent, pair_landed, partner)
        line = factor.at[:, (x + 4 - d) % 4, core, :, right]
        drain(line, far_landed.at[1, d])
        send(line, line, pair_sent, pair_landed, partner)

    for e in range(1, per_device):
        spread_strip(e)
    for copy in kept:
        copy.start()

    drain(factor.at[:, :, 0], pair_landed)

    spike = factor[0, 0, 0, 0:1, :]
    columns = lax.broadcasted_iota(jnp.int32, (1, W), 1)
    spike_row = jnp.where(columns < W - deflated[0], spike, 0.0)
    squares = jnp.sum(spike_row * spike_row, axis=1, keepdims=True)
    corner = spike[:, 0:1]
    magnitude = jnp.sqrt(squares + 1e-06)
    signum = jnp.where(corner >= 0, 1.0, -1.0)
    vector = spike_row + jnp.where(columns == 0, signum * magnitude, 0.0)
    denominator = squares + 2.0 * jnp.abs(corner) * magnitude + magnitude * magnitude
    scaling = 2.0 / denominator

    @pl.loop(0, ROWS, unroll=4)
    def _(b):
        block = factor[b // 8, (b // 2) % 4, b % 2]
        image = jnp.sum(block * vector, axis=1, keepdims=True)
        turned = block - (scaling * image) * vector
        top = turned.astype(jnp.bfloat16)
        high[pl.ds(pl.multiple_of(b * 32, 32), 32), :] = top
        low[pl.ds(pl.multiple_of(b * 32, 32), 32), :] = (turned - top.astype(jnp.float32)).astype(jnp.bfloat16)

    def turn(first, count):
        some = pl.ds(first, count)
        shape = (count, 8, 256)
        number = (
            ((first - ROUNDS + lax.broadcasted_iota(jnp.int32, shape, 0)) * ROWS + row) * 64
            + mine * 8 + lax.broadcasted_iota(jnp.int32, shape, 1)
        )

        def store(columns, value):
            x_out[some, :, columns] = jnp.where(number < start, value.reshape(shape), x_in[some, :, columns])

        rotate(x_in[some].reshape(count * 8, W), high, low, store)

        def give(target, base, side):
            where = pl.ds(first - base, count)
            over_z(lambda other: send(
                x_out.at[some, :, lanes(other)], target.at[where, mine],
                out_sent.at[side], out_landed.at[side], (row, other),
            ))
            pltpu.make_async_copy(x_out.at[some, :, lanes(mine)], target.at[where, mine], local.at[5]).start()

        if isinstance(first, int):
            give(co_ref, ROUNDS, 1)
        else:
            pl.when(first < ROUNDS)(lambda: give(zo_ref, 0, 0))
            pl.when(first >= ROUNDS)(lambda: give(co_ref, ROUNDS, 1))

    def turn_strip():
        @pl.loop(0, per_device)
        def _(e):
            drain(s_in.at[0, 0:992], s_landed.at[e])
            pltpu.make_async_copy(
                s_ref.at[:, first_round + row * per_device + e], s_in.at[e, pl.ds(row * 32, 32)], local.at[3 + e]
            ).wait()

            @pl.loop(0, 8)
            def _(k):
                s_turned[:, lanes(k)] = s_in[e, pl.ds(pl.multiple_of(k * 128, 128), 128), 0, :].T

            number = (
                ((first_round + row * per_device + e) * Z + mine) * 128
                + lax.broadcasted_iota(jnp.int32, (128, 256), 0)
            )

            def store(columns, value):
                s_rotated[:, columns] = jnp.where(number >= start + W, value, s_turned[:, columns])

            rotate(s_turned[...], high, low, store)

            @pl.loop(0, 8)
            def _(k):
                s_out[e, pl.ds(pl.multiple_of(k * 128, 128), 128), 0, :] = s_rotated[:, lanes(k)].T

            @pl.loop(1, ROWS)
            def _(d):
                other = (row + d) % ROWS
                send(
                    s_out.at[e, pl.ds(other * 32, 32)],
                    so_ref.at[:, first_round + row * per_device + e],
                    so_sent, so_landed, (other, mine),
                )

            pltpu.make_async_copy(
                s_out.at[e, pl.ds(row * 32, 32)], so_ref.at[:, first_round + row * per_device + e], local.at[6 + e]
            ).start()

        own[1].wait()
        drain(x_in.at[ROUNDS:total, :, 0:896], in_landed.at[1])

    own_results = [
        pltpu.make_async_copy(
            s_out.at[e, pl.ds(row * 32, 32)], so_ref.at[:, first_round + row * per_device + e], local.at[6 + e]
        )
        for e in range(per_device)
    ]
    own[0].wait()
    drain(x_in.at[0:ROUNDS, :, 0:896], in_landed.at[0])

    @pl.loop(0, total // 8)
    def _(c):
        if rounds >= 8:
            pl.when(c == ROUNDS // 8)(turn_strip)
        turn(pl.multiple_of(c * 8, 8), 8)

    if rounds < 8:
        turn_strip()
    if total % 8:
        turn(total - total % 8, total % 8)
    drain(x_out.at[0:total, :, 0:128], local.at[5])

    for copy in own_results + kept:
        copy.wait()
    drain(factor.at[0, 0, 0, :, 0:896], f_sent)
    for side in range(2):
        drain(factor.at[0, 0:3, 0, :, left], ring_sent.at[side])
        drain(factor.at[0:3, :, 0, :, left], far_sent.at[side])
    drain(factor.at[:, :, 0], pair_sent)
    drain(s_in.at[0:per_device, 0:992], s_sent)
    drain(s_in.at[0:per_device, 0:992], so_sent)
    drain(s_in.at[0:per_device, 0:992], so_landed)
    for side, part in enumerate((slice(0, ROUNDS), slice(ROUNDS, total))):
        for semaphores in (in_sent, out_sent, out_landed):
            drain(x_in.at[part, :, 0:896], semaphores.at[side])


def variant(rounds):
    per_device, first_round = (2, 0) if rounds <= 16 else (1, 32)
    anywhere = pl.BlockSpec(memory_space=pl.ANY)
    blocks = jax.ShapeDtypeStruct((ROUNDS, Z, 8, 128), jnp.float32)
    dma = pltpu.SemaphoreType.DMA
    return pl.pallas_call(
        functools.partial(kernel, rounds, per_device, first_round),
        name=f"window_{rounds}",
        out_shape=(blocks, blocks, jax.ShapeDtypeStruct((32, 64, 1, 128), jnp.float32)),
        in_specs=[*[pl.BlockSpec(memory_space=pltpu.SMEM)] * 2, *[pl.BlockSpec(memory_space=pltpu.HBM)] * 4],
        out_specs=(anywhere, anywhere, anywhere),
        scratch_shapes=[
            pltpu.VMEM((4, 4, 2, 32, W), jnp.float32),
            pltpu.VMEM((W, W), jnp.bfloat16),
            pltpu.VMEM((W, W), jnp.bfloat16),
            *[pltpu.VMEM((2 * ROUNDS, 8, W), jnp.float32) for _ in range(2)],
            *[pltpu.VMEM((2, W, 1, 128), jnp.float32) for _ in range(2)],
            *[pltpu.VMEM((128, W), jnp.float32) for _ in range(2)],
            dma((10,)),
            dma, dma, dma((2,)), dma((2, 4)), dma((2,)), dma((2, 4)), dma, dma,
            dma((2,)), dma((2,)), dma((2,)), dma((2,)), dma, dma((2,)), dma, dma,
        ],
        compiler_params=pltpu.CompilerParams(
            collective_id=rounds // STEP, has_side_effects=True, vmem_limit_bytes=48 * 1024 * 1024
        ),
    )


def put_down(*arrays):
    def copies(*refs):
        sources, targets, semaphores = refs[: len(arrays)], refs[len(arrays): -1], refs[-1]
        moves = [
            pltpu.make_async_copy(source.at[pl.ds(8 * part, 8)], target.at[pl.ds(8 * part, 8)], semaphores.at[n, part])
            for n, (source, target) in enumerate(zip(sources, targets))
            for part in range(4)
        ]
        for move in moves:
            move.start()
        for move in moves:
            move.wait()

    anywhere = [pl.BlockSpec(memory_space=pl.ANY)] * len(arrays)
    return pl.pallas_call(
        copies,
        name="put_down",
        out_shape=tuple(jax.ShapeDtypeStruct(array.shape, array.dtype) for array in arrays),
        in_specs=anywhere,
        out_specs=anywhere,
        scratch_shapes=[pltpu.SemaphoreType.DMA((len(arrays), 4))],
    )(*arrays)


def body(vectors_window, column_strip, row_strip, factor, window_start, deflated):
    start = window_start[0]
    by_worker = (ROUNDS, Z, 8, 128)
    vectors, strip, rows = lax.switch(
        (start - 1) // (64 * ROWS * STEP),
        [variant(rounds) for rounds in range(STEP, ROUNDS + 1, STEP)],
        window_start, deflated, pltpu.with_memory_space_constraint(factor, pltpu.HBM),
        vectors_window.reshape(by_worker), column_strip.reshape(by_worker), row_strip,
    )
    vectors, strip, rows = put_down(vectors, strip, rows)
    return vectors.reshape(vectors_window.shape), strip.reshape(column_strip.shape), rows


def solution(mesh):
    return jax.shard_map(
        body,
        mesh=mesh,
        in_specs=(
            P(None, "row", None, "col"),
            P(None, "row", None, "col"),
            P("row", None, "col", None),
            P("row", "col"),
            P(),
            P(),
        ),
        out_specs=(
            P(None, "row", None, "col"),
            P(None, "row", None, "col"),
            P("row", None, "col", None),
        ),
        check_vma=False,
    )
```

```python
import functools

import jax
import jax.numpy as jnp
from jax import lax
from jax.experimental import pallas as pl
from jax.experimental.pallas import tpu as pltpu
from jax.sharding import PartitionSpec as P

W = 1024
Z = 8
ROWS = 32
ROUNDS = 32
STEP = 2
MESH = pl.DeviceIdType.MESH


def send(src, dst, sent, landed, device):
    pltpu.make_async_remote_copy(
        src_ref=src, dst_ref=dst, send_sem=sent, recv_sem=landed, device_id=device, device_id_type=MESH
    ).start()


def drain(ref, semaphore):
    pltpu.make_async_copy(ref, ref, semaphore).wait()


def lanes(index, size=128):
    return pl.ds(pl.multiple_of(index * size, size), size)


def row_of(y, x, core):
    return (y * 4 + x) * 2 + core


def rotate(x, high, low, store):
    rows = x.shape[0]
    x_high = x.astype(jnp.bfloat16)
    x_low = (x - x_high.astype(jnp.float32)).astype(jnp.bfloat16)
    both = jnp.concatenate([x_high, x_low], axis=0)

    @pl.loop(0, 4, unroll=1)
    def _(n):
        columns = lanes(n, 256)
        top = jnp.dot(both, high[:, columns], preferred_element_type=jnp.float32)
        bottom = jnp.dot(x_high, low[:, columns], preferred_element_type=jnp.float32)
        store(columns, top[:rows] + top[rows:] + bottom)


def kernel(
    rounds, per_device, first_round,
    starts, deflated, f_ref, z_ref, c_ref, s_ref,
    zo_ref, co_ref, so_ref,
    factor, high, low, x_in, x_out, s_in, s_out, s_turned, s_rotated,
    local, f_sent, f_landed, ring_sent, ring_landed, far_sent, far_landed, pair_sent, pair_landed,
    in_sent, in_landed, out_sent, out_landed, s_sent, s_landed, so_sent, so_landed,
):
    row = lax.axis_index("row")
    mine = lax.axis_index("col")
    y, x, core = row // 8, (row // 2) % 4, row % 2
    barrier = pltpu.get_barrier_semaphore()
    own_factor = factor.at[y, x, core, :, lanes(mine)]
    load = pltpu.make_async_copy(f_ref, own_factor, local.at[0])
    load.start()

    @pl.loop(1, Z)
    def _(d):
        pl.semaphore_signal(barrier, inc=1, device_id=(row, (mine + d) % Z), device_id_type=MESH)

    @pl.loop(1, ROWS)
    def _(d):
        pl.semaphore_signal(barrier, inc=1, device_id=((row + d) % ROWS, mine), device_id_type=MESH)

    start = starts[0]
    total = ROUNDS + rounds
    untouched = []
    if rounds < ROUNDS:
        untouched.append((c_ref.at[rounds:], co_ref.at[rounds:]))
    if first_round:
        untouched.append((s_ref.at[:, 0:first_round], so_ref.at[:, 0:first_round]))
    own = [
        pltpu.make_async_copy(z_ref.at[:, mine], x_in.at[0:ROUNDS, :, lanes(mine)], local.at[1]),
        pltpu.make_async_copy(c_ref.at[0:rounds, mine], x_in.at[ROUNDS:total, :, lanes(mine)], local.at[2]),
    ]
    for copy in own:
        copy.start()
    kept = [pltpu.make_async_copy(source, target, local.at[8 + n]) for n, (source, target) in enumerate(untouched)]
    load.wait()
    pl.semaphore_wait(barrier, Z - 1 + ROWS - 1)

    def over_z(move):
        @pl.loop(0, Z - 1)
        def _(i):
            move((mine + 4 + (1 - 2 * (i % 2)) * ((i + 1) // 2)) % Z)

    def in_order(move):
        @pl.loop(0, Z - 1)
        def _(i):
            move(i + jnp.where(i >= mine, 1, 0))

    over_z(lambda other: send(own_factor, own_factor, f_sent, f_landed, (row, other)))
    over_z(lambda other: send(
        z_ref.at[:, other], x_in.at[0:ROUNDS, :, lanes(mine)], in_sent.at[0], in_landed.at[0], (row, other)
    ))
    own_rounds = [
        pltpu.make_async_copy(
            s_ref.at[:, first_round + row * per_device + e], s_in.at[e, pl.ds(row * 32, 32)], local.at[3 + e]
        )
        for e in range(per_device)
    ]

    def spread_strip(e):
        @pl.loop(1, ROWS)
        def _(d):
            other = (row + d) % ROWS
            send(
                s_ref.at[:, first_round + other * per_device + e],
                s_in.at[e, pl.ds(row * 32, 32)],
                s_sent, s_landed.at[e], (other, mine),
            )

        own_rounds[e].start()

    spread_strip(0)
    over_z(lambda other: send(
        c_ref.at[0:rounds, other], x_in.at[ROUNDS:total, :, lanes(mine)],
        in_sent.at[1], in_landed.at[1], (row, other),
    ))

    left, right = slice(0, 512), slice(512, 1024)
    partner = (row_of(y, x, 1 - core), mine)

    def along_x(d):
        return row_of(y, (x + d) % 4, core), mine

    def along_y(d):
        return row_of((y + d) % 4, x, core), mine

    def forward(piece, side, across):
        @pl.loop(0, 3)
        def _(i):
            d = (i + 1) % 3 + 1
            send(piece, piece, far_sent.at[side], far_landed.at[side, d], across(d))

    drain(factor.at[0, 0, 0, :, 0:896], f_landed)
    piece_left, piece_right = factor.at[y, x, core, :, left], factor.at[y, x, core, :, right]

    @pl.loop(0, 3)
    def _(i):
        d = (i + 1) % 3 + 1
        send(piece_left, piece_left, ring_sent.at[0], ring_landed.at[0, d], along_x(d))
        send(piece_right, piece_right, ring_sent.at[1], ring_landed.at[1, d], along_y(d))

    forward(piece_left, 0, along_y)
    forward(piece_right, 1, along_x)
    send(piece_left, piece_left, pair_sent, pair_landed, partner)
    send(piece_right, piece_right, pair_sent, pair_landed, partner)

    @pl.loop(0, 3)
    def _(i):
        e = 1 + i * 2 - 3 * (i // 2)
        piece = factor.at[y, (x + 4 - e) % 4, core, :, left]
        drain(piece, ring_landed.at[0, e])
        forward(piece, 0, along_y)
        send(piece, piece, pair_sent, pair_landed, partner)
        piece = factor.at[(y + 4 - e) % 4, x, core, :, right]
        drain(piece, ring_landed.at[1, e])
        forward(piece, 1, along_x)
        send(piece, piece, pair_sent, pair_landed, partner)

    @pl.loop(0, 3)
    def _(i):
        d = 1 + i * 2 - 3 * (i // 2)
        line = factor.at[(y + 4 - d) % 4, :, core, :, left]
        drain(line, far_landed.at[0, d])
        send(line, line, pair_sent, pair_landed, partner)
        line = factor.at[:, (x + 4 - d) % 4, core, :, right]
        drain(line, far_landed.at[1, d])
        send(line, line, pair_sent, pair_landed, partner)

    for e in range(1, per_device):
        spread_strip(e)
    for copy in kept:
        copy.start()

    drain(factor.at[:, :, 0], pair_landed)

    spike = factor[0, 0, 0, 0:1, :]
    columns = lax.broadcasted_iota(jnp.int32, (1, W), 1)
    spike_row = jnp.where(columns < W - deflated[0], spike, 0.0)
    squares = jnp.sum(spike_row * spike_row, axis=1, keepdims=True)
    corner = spike[:, 0:1]
    magnitude = jnp.sqrt(squares + 1e-06)
    signum = jnp.where(corner >= 0, 1.0, -1.0)
    vector = spike_row + jnp.where(columns == 0, signum * magnitude, 0.0)
    denominator = squares + 2.0 * jnp.abs(corner) * magnitude + magnitude * magnitude
    scaling = 2.0 / denominator

    @pl.loop(0, ROWS, unroll=8)
    def _(b):
        block = factor[b // 8, (b // 2) % 4, b % 2]
        image = jnp.sum(block * vector, axis=1, keepdims=True)
        turned = block - (scaling * image) * vector
        top = turned.astype(jnp.bfloat16)
        high[pl.ds(pl.multiple_of(b * 32, 32), 32), :] = top
        low[pl.ds(pl.multiple_of(b * 32, 32), 32), :] = (turned - top.astype(jnp.float32)).astype(jnp.bfloat16)

    def turn(first, count):
        some = pl.ds(first, count)
        shape = (count, 8, 256)
        number = (
            ((first - ROUNDS + lax.broadcasted_iota(jnp.int32, shape, 0)) * ROWS + row) * 64
            + mine * 8 + lax.broadcasted_iota(jnp.int32, shape, 1)
        )

        def store(columns, value):
            x_out[some, :, columns] = jnp.where(number < start, value.reshape(shape), x_in[some, :, columns])

        rotate(x_in[some].reshape(count * 8, W), high, low, store)

        def give(target, base, side):
            where = pl.ds(first - base, count)
            (in_order if side else over_z)(lambda other: send(
                x_out.at[some, :, lanes(other)], target.at[where, mine],
                out_sent.at[side], out_landed.at[side], (row, other),
            ))
            pltpu.make_async_copy(x_out.at[some, :, lanes(mine)], target.at[where, mine], local.at[5]).start()

        if isinstance(first, int):
            give(co_ref, ROUNDS, 1)
        else:
            pl.when(first < ROUNDS)(lambda: give(zo_ref, 0, 0))
            pl.when(first >= ROUNDS)(lambda: give(co_ref, ROUNDS, 1))

    def turn_strip():
        @pl.loop(0, per_device)
        def _(e):
            drain(s_in.at[0, 0:992], s_landed.at[e])
            pltpu.make_async_copy(
                s_ref.at[:, first_round + row * per_device + e], s_in.at[e, pl.ds(row * 32, 32)], local.at[3 + e]
            ).wait()

            @pl.loop(0, 8)
            def _(k):
                s_turned[:, lanes(k)] = s_in[e, pl.ds(pl.multiple_of(k * 128, 128), 128), 0, :].T

            number = (
                ((first_round + row * per_device + e) * Z + mine) * 128
                + lax.broadcasted_iota(jnp.int32, (128, 256), 0)
            )

            def store(columns, value):
                s_rotated[:, columns] = jnp.where(number >= start + W, value, s_turned[:, columns])

            rotate(s_turned[...], high, low, store)

            @pl.loop(0, 8)
            def _(k):
                s_out[e, pl.ds(pl.multiple_of(k * 128, 128), 128), 0, :] = s_rotated[:, lanes(k)].T

            @pl.loop(1, ROWS)
            def _(d):
                other = (row + d) % ROWS
                send(
                    s_out.at[e, pl.ds(other * 32, 32)],
                    so_ref.at[:, first_round + row * per_device + e],
                    so_sent, so_landed, (other, mine),
                )

            pltpu.make_async_copy(
                s_out.at[e, pl.ds(row * 32, 32)], so_ref.at[:, first_round + row * per_device + e], local.at[6 + e]
            ).start()

        own[1].wait()
        drain(x_in.at[ROUNDS:total, :, 0:896], in_landed.at[1])

    own_results = [
        pltpu.make_async_copy(
            s_out.at[e, pl.ds(row * 32, 32)], so_ref.at[:, first_round + row * per_device + e], local.at[6 + e]
        )
        for e in range(per_device)
    ]
    own[0].wait()
    drain(x_in.at[0:ROUNDS, :, 0:896], in_landed.at[0])

    @pl.loop(0, total // 8)
    def _(c):
        if rounds >= 8:
            pl.when(c == ROUNDS // 8)(turn_strip)
        turn(pl.multiple_of(c * 8, 8), 8)

    if rounds < 8:
        turn_strip()
    if total % 8:
        turn(total - total % 8, total % 8)
    drain(x_out.at[0:total, :, 0:128], local.at[5])

    for copy in own_results + kept:
        copy.wait()
    drain(factor.at[0, 0, 0, :, 0:896], f_sent)
    for side in range(2):
        drain(factor.at[0, 0:3, 0, :, left], ring_sent.at[side])
        drain(factor.at[0:3, :, 0, :, left], far_sent.at[side])
    drain(factor.at[:, :, 0], pair_sent)
    drain(s_in.at[0:per_device, 0:992], s_sent)
    drain(s_in.at[0:per_device, 0:992], so_sent)
    drain(s_in.at[0:per_device, 0:992], so_landed)
    for side, part in enumerate((slice(0, ROUNDS), slice(ROUNDS, total))):
        for semaphores in (in_sent, out_sent, out_landed):
            drain(x_in.at[part, :, 0:896], semaphores.at[side])


def variant(rounds):
    per_device, first_round = (2, 0) if rounds <= 16 else (1, 32)
    anywhere = pl.BlockSpec(memory_space=pl.ANY)
    blocks = jax.ShapeDtypeStruct((ROUNDS, Z, 8, 128), jnp.float32)
    dma = pltpu.SemaphoreType.DMA
    return pl.pallas_call(
        functools.partial(kernel, rounds, per_device, first_round),
        name=f"window_{rounds}",
        out_shape=(blocks, blocks, jax.ShapeDtypeStruct((32, 64, 1, 128), jnp.float32)),
        in_specs=[*[pl.BlockSpec(memory_space=pltpu.SMEM)] * 2, *[pl.BlockSpec(memory_space=pltpu.HBM)] * 4],
        out_specs=(anywhere, anywhere, anywhere),
        scratch_shapes=[
            pltpu.VMEM((4, 4, 2, 32, W), jnp.float32),
            pltpu.VMEM((W, W), jnp.bfloat16),
            pltpu.VMEM((W, W), jnp.bfloat16),
            *[pltpu.VMEM((2 * ROUNDS, 8, W), jnp.float32) for _ in range(2)],
            *[pltpu.VMEM((2, W, 1, 128), jnp.float32) for _ in range(2)],
            *[pltpu.VMEM((128, W), jnp.float32) for _ in range(2)],
            dma((10,)),
            dma, dma, dma((2,)), dma((2, 4)), dma((2,)), dma((2, 4)), dma, dma,
            dma((2,)), dma((2,)), dma((2,)), dma((2,)), dma, dma((2,)), dma, dma,
        ],
        compiler_params=pltpu.CompilerParams(
            collective_id=rounds // STEP, has_side_effects=True, vmem_limit_bytes=48 * 1024 * 1024
        ),
    )


def put_down(*arrays):
    def copies(*refs):
        sources, targets, semaphores = refs[: len(arrays)], refs[len(arrays): -1], refs[-1]
        moves = [
            pltpu.make_async_copy(source.at[pl.ds(8 * part, 8)], target.at[pl.ds(8 * part, 8)], semaphores.at[n, part])
            for n, (source, target) in enumerate(zip(sources, targets))
            for part in range(4)
        ]
        for move in moves:
            move.start()
        for move in moves:
            move.wait()

    anywhere = [pl.BlockSpec(memory_space=pl.ANY)] * len(arrays)
    return pl.pallas_call(
        copies,
        name="put_down",
        out_shape=tuple(jax.ShapeDtypeStruct(array.shape, array.dtype) for array in arrays),
        in_specs=anywhere,
        out_specs=anywhere,
        scratch_shapes=[pltpu.SemaphoreType.DMA((len(arrays), 4))],
    )(*arrays)


def body(vectors_window, column_strip, row_strip, factor, window_start, deflated):
    start = window_start[0]
    by_worker = (ROUNDS, Z, 8, 128)
    vectors, strip, rows = lax.switch(
        (start - 1) // (64 * ROWS * STEP),
        [variant(rounds) for rounds in range(STEP, ROUNDS + 1, STEP)],
        window_start, deflated, pltpu.with_memory_space_constraint(factor, pltpu.HBM),
        vectors_window.reshape(by_worker), column_strip.reshape(by_worker), row_strip,
    )
    vectors, strip, rows = put_down(vectors, strip, rows)
    return vectors.reshape(vectors_window.shape), strip.reshape(column_strip.shape), rows


def solution(mesh):
    return jax.shard_map(
        body,
        mesh=mesh,
        in_specs=(
            P(None, "row", None, "col"),
            P(None, "row", None, "col"),
            P("row", None, "col", None),
            P("row", "col"),
            P(),
            P(),
        ),
        out_specs=(
            P(None, "row", None, "col"),
            P(None, "row", None, "col"),
            P("row", None, "col", None),
        ),
        check_vma=False,
    )
```
